32 devices in a mesh: lon: 8 (over y, x, core), lat: 4 (over z).
Axes of the slice: x: 2, y: 2, z: 4, core: 2. Of those that a mesh axis runs over, the one named last changes fastest.
Arguments:
- grid_state: bfloat16 [8, 4, 512, 227], P('lon', 'lat'), may hold values from -6 to 6
- grid_weight: bfloat16 [227, 512], replicated, may hold values from -0.375 to 0.375
- encode_weights: bfloat16 [2, 512, 512], replicated, may hold values from -0.25 to 0.25
- encode_bias: float32 [512], replicated, may hold values from -3 to 3
- mesh_gain: float32 [512], replicated, may hold values from 0.25 to 1.75
- g2m_sender: int32 [8, 4, 512], P('lon', 'lat'), may hold values from 0 to 511
- g2m_receiver: int32 [8, 4, 512], P('lon', 'lat'), may hold values from 0 to 255, as said below
- edge_geometry: float32 [8, 4, 4, 1536], P('lon', 'lat'), may hold values from -6 to 6
- edge_embed: float32 [4, 512], replicated, may hold values from -3 to 3
- mesh_sender: int32 [8, 4, 1536], P('lon', 'lat'), may hold values from 0 to 543, as said below
- mesh_receiver: int32 [8, 4, 1536], P('lon', 'lat'), may hold values from 0 to 255
- block_count: int32 [8, 4], P('lon', 'lat'), may hold values from 1 to 6, as said below
- export_nodes: int32 [8, 4, 32], P('lon', 'lat'), may hold values from 0 to 255, as said below
- proc_weights: bfloat16 [2, 7, 512, 512], replicated, may hold values from -0.25 to 0.25
- proc_bias: float32 [2, 2, 512], replicated, may hold values from -3 to 3
- proc_gain: float32 [2, 2, 512], replicated, may hold values from 0.25 to 1.75
- mesh_cotangent: bfloat16 [8, 4, 256, 512], P('lon', 'lat'), may hold values from -6 to 6
Outputs:
- mesh_latents: bfloat16 [8, 4, 256, 512], P('lon', 'lat')
- weight_grads: float32 [2, 32, 57344], P(None, ('lon', 'lat'))
- latent_grad: bfloat16 [8, 4, 256, 512], P('lon', 'lat')
The draws below stay inside these ranges and needn't reach their ends.
Inputs may be any that keep to these rules, and one draw needn't show every extreme that they name: `g2m_receiver`: every one of a device's 256 mesh nodes is the receiver of at least one of its grid-to-mesh edges. `mesh_sender`: an index below 256 names an own node; 256 + g * 32 + r names row r of export_nodes of the device v bands and w sectors away, g = 3 * (v + 1) + (w + 1), v and w in -1..1, never both 0, never beyond the first or last band; sectors wrap around. Blocks at or beyond block_count hold padding edges that are ignored. `export_nodes`: 32 different own nodes.
All inputs are finite; a program needn't handle non-finite values.
Results may differ from the reference program's by a relative error of at most 0.02.
Values may be sent and summed in bfloat16 or wider, within the bound.
A program may use at most 128 MiB of HBM per device.

```python
from functools import partial
import jax
import jax.numpy as jnp
from jax import lax

D = 512
C = 227
M_DEV = 256
STEPS = 2
EDGE_BLOCK = 256
G_DEV = 512
B_DEV = 32
G2M_BLK = 2
E_CAP = 6
SECTORS = 8
BANDS = 4


def draw_g2m_receiver(key, part):
    edge_total = G2M_BLK * EDGE_BLOCK
    keys = jax.random.split(jax.random.fold_in(key, 11), SECTORS * BANDS)

    def one_device(device_key):
        first_key, second_key, third_key = jax.random.split(device_key, 3)
        covering = jax.random.permutation(first_key, M_DEV).astype(jnp.int32)
        filler = jax.random.randint(second_key, (edge_total - M_DEV,), 0, M_DEV, dtype=jnp.int32)
        joined = jnp.concatenate([covering, filler])
        return jnp.take(joined, jax.random.permutation(third_key, edge_total), axis=0)
    return jax.vmap(one_device)(keys).reshape(SECTORS, BANDS, edge_total).astype(jnp.int32)


def draw_mesh_sender(key, part):
    grid_shape = (SECTORS, BANDS, E_CAP * EDGE_BLOCK)
    first_key, second_key, third_key, fourth_key = jax.random.split(jax.random.fold_in(key, 23), 4)
    choose = jax.random.randint(first_key, grid_shape, 0, 5, dtype=jnp.int32)
    local_node = jax.random.randint(second_key, grid_shape, 0, M_DEV, dtype=jnp.int32)
    picked = jax.random.randint(third_key, grid_shape, 0, 8, dtype=jnp.int32)
    slot_index = picked + (picked >= 4).astype(jnp.int32)
    row_index = jax.random.randint(fourth_key, grid_shape, 0, B_DEV, dtype=jnp.int32)
    band_index = lax.broadcasted_iota(jnp.int32, grid_shape, 1)
    vertical = slot_index // 3 - 1
    lateral = slot_index % 3 - 1
    vertical = jnp.where((band_index == 0) & (vertical < 0), 1, vertical)
    vertical = jnp.where((band_index == BANDS - 1) & (vertical > 0), -1, vertical)
    slot_index = (vertical + 1) * 3 + lateral + 1
    remote = M_DEV + slot_index * B_DEV + row_index
    return jnp.where(choose < 3, local_node, remote).astype(jnp.int32)


def draw_block_count(key, part):
    band_index = lax.broadcasted_iota(jnp.int32, (SECTORS, BANDS), 1)
    sector_index = lax.broadcasted_iota(jnp.int32, (SECTORS, BANDS), 0)
    distance = jnp.abs(2 * band_index + 1 - BANDS)
    base_count = E_CAP - (distance - 1) * (E_CAP - 1) // max(BANDS - 2, 1)
    jitter = jax.random.randint(jax.random.fold_in(key, 31), (SECTORS, BANDS), 0, 2, dtype=jnp.int32)
    moved = jnp.where(base_count >= E_CAP, base_count - jitter, base_count + jitter)
    moved = jnp.where(sector_index == 0, base_count, moved)
    return jnp.clip(moved, 1, E_CAP).astype(jnp.int32)


def draw_export_nodes(key, part):
    keys = jax.random.split(jax.random.fold_in(key, 47), SECTORS * BANDS)

    def one_device(device_key):
        return jax.random.permutation(device_key, M_DEV)[:B_DEV].astype(jnp.int32)
    return jax.vmap(one_device)(keys).reshape(SECTORS, BANDS, B_DEV).astype(jnp.int32)


def set_ends(result, own_key, smallest, high):
    longest = result.shape.index(max(result.shape))
    spots = []
    for shift in (0, 1):
        where = [jax.random.randint(jax.random.fold_in(own_key, axis), (), 0, length) for axis, length in enumerate(result.shape)]
        where[longest] = (where[longest] + shift) % result.shape[longest]
        spots.append(tuple(where))
    return result.at[spots[0]].set(smallest).at[spots[1]].set(high)


def shard_levels(rng, extent, shards, least, top_value):
    level = 1.0
    for dim, shards_of in shards:
        draws = jax.random.uniform(jax.random.fold_in(jax.random.fold_in(rng, 6), dim), (shards_of,), jnp.float32, least / len(shards), top_value / len(shards))
        level = level * jnp.repeat(jnp.exp(draws), extent[dim] // shards_of).reshape((-1,) + (1,) * (len(extent) - 1 - dim))
    return level


def normal_values(key, dims, deviation, bound, pieces=(), kind=jnp.bfloat16):
    level = shard_levels(key, dims, pieces, -0.22, 0.18) if pieces else 1.0
    drawn = jax.random.normal(key, dims, jnp.float32) * deviation * level
    return jnp.minimum(jnp.maximum(drawn, -bound), bound).astype(kind)


def setup_inputs(seed: int = 0) -> dict:
    streams_of = jax.random.split(jax.random.key(seed), 18)
    return {
        "grid_state": normal_values(streams_of[0], (SECTORS, BANDS, G_DEV, C), 1.0, 6.0, ((0, 8), (1, 4))),
        "grid_weight": normal_values(streams_of[1], (C, D), C ** -0.5, 0.375),
        "encode_weights": normal_values(streams_of[2], (2, D, D), D ** -0.5, 0.25),
        "encode_bias": normal_values(streams_of[3], (D,), 0.5, 3.0, (), jnp.float32),
        "mesh_gain": jnp.clip(1.0 + 0.15 * jax.random.normal(streams_of[4], (D,), jnp.float32), 0.25, 1.75),
        "g2m_sender": set_ends(jax.random.randint(streams_of[5], (SECTORS, BANDS, G2M_BLK * EDGE_BLOCK), 0, G_DEV), jax.random.fold_in(streams_of[5], 1), 0, G_DEV - 1).astype(jnp.int32),
        "g2m_receiver": draw_g2m_receiver(jax.random.fold_in(streams_of[17], 71), 0),
        "edge_geometry": normal_values(streams_of[7], (SECTORS, BANDS, 4, E_CAP * EDGE_BLOCK), 1.0, 6.0, ((0, 8), (1, 4)), jnp.float32),
        "edge_embed": normal_values(streams_of[8], (4, D), 4 ** -0.5, 3.0, (), jnp.float32),
        "mesh_sender": draw_mesh_sender(jax.random.fold_in(streams_of[17], 71), 0),
        "mesh_receiver": set_ends(jax.random.randint(streams_of[10], (SECTORS, BANDS, E_CAP * EDGE_BLOCK), 0, M_DEV), jax.random.fold_in(streams_of[10], 1), 0, M_DEV - 1).astype(jnp.int32),
        "block_count": draw_block_count(jax.random.fold_in(streams_of[17], 71), 0),
        "export_nodes": draw_export_nodes(jax.random.fold_in(streams_of[17], 71), 0),
        "proc_weights": normal_values(streams_of[13], (STEPS, 7, D, D), D ** -0.5, 0.25),
        "proc_bias": normal_values(streams_of[14], (STEPS, 2, D), 0.5, 3.0, (), jnp.float32),
        "proc_gain": jnp.clip(1.0 + 0.15 * jax.random.normal(streams_of[15], (STEPS, 2, D), jnp.float32), 0.25, 1.75),
        "mesh_cotangent": normal_values(streams_of[16], (SECTORS, BANDS, M_DEV, D), 1.0, 6.0, ((0, 8), (1, 4))),
    }


EPSILON = 1e-05

def layer_norm(values):
    average = lax.optimization_barrier(jnp.mean(values, axis=-1, keepdims=True))
    centred = values - average
    variance = lax.optimization_barrier(jnp.mean(centred * centred, axis=-1, keepdims=True))
    return centred * lax.rsqrt(variance + EPSILON)

def encode(grid_rows, grid_weight, encode_weights, encode_bias, mesh_gain, g2m_sender, g2m_receiver, node_count):
    grid_latent = jax.nn.silu(jnp.dot(grid_rows, grid_weight, preferred_element_type=jnp.float32)).astype(jnp.bfloat16)
    projected = jnp.dot(grid_latent, encode_weights[0], preferred_element_type=jnp.float32)
    message_act = jax.nn.silu(jnp.take(projected, g2m_sender, axis=0) + encode_bias).astype(jnp.bfloat16)
    message = jnp.dot(message_act, encode_weights[1], preferred_element_type=jnp.float32).astype(jnp.bfloat16)
    onehot = (g2m_receiver[:, None] == jnp.arange(node_count, dtype=jnp.int32)[None, :]).astype(jnp.bfloat16)
    gathered = lax.dot_general(onehot, message, (((0,), (0,)), ((), ())), preferred_element_type=jnp.float32)
    return (layer_norm(gathered) * mesh_gain).astype(jnp.bfloat16)

def embed_edges(geometry, edge_embed):
    product = lax.dot_general(geometry, edge_embed, (((0,), (0,)), ((), ())), precision=lax.Precision.HIGHEST, preferred_element_type=jnp.float32)
    return product.astype(jnp.bfloat16)

def mesh_step(latent, halo_rows, edge_state, weights, sender, receiver, live_mask, bias, gain):
    node_count = latent.shape[0]
    extended = jnp.concatenate([latent, halo_rows], axis=0).astype(jnp.bfloat16)
    sender_proj = jnp.dot(extended, weights[1], preferred_element_type=jnp.float32)
    own_rows = latent.astype(jnp.bfloat16)
    receiver_proj = jnp.dot(own_rows, weights[2], preferred_element_type=jnp.float32)
    before = jnp.dot(edge_state, weights[0], preferred_element_type=jnp.float32)
    before = before + jnp.take(sender_proj, sender, axis=0) + jnp.take(receiver_proj, receiver, axis=0) + bias[0]
    edge_act = jax.nn.silu(before).astype(jnp.bfloat16)
    update = layer_norm(jnp.dot(edge_act, weights[3], preferred_element_type=jnp.float32)) * gain[0] * live_mask[:, None]
    new_edges = (edge_state.astype(jnp.float32) + update).astype(jnp.bfloat16)
    onehot = (receiver[:, None] == jnp.arange(node_count, dtype=jnp.int32)[None, :]).astype(jnp.bfloat16)
    node_sum = lax.dot_general(onehot, update.astype(jnp.bfloat16), (((0,), (0,)), ((), ())), preferred_element_type=jnp.float32).astype(jnp.bfloat16)
    inner = jnp.dot(own_rows, weights[4], preferred_element_type=jnp.float32)
    inner = inner + jnp.dot(node_sum, weights[5], preferred_element_type=jnp.float32) + bias[1]
    node_act = jax.nn.silu(inner).astype(jnp.bfloat16)
    new_latent = latent + layer_norm(jnp.dot(node_act, weights[6], preferred_element_type=jnp.float32)) * gain[1]
    return (new_latent, new_edges)

def band_shift(values, offset):
    if offset == 0:
        return values
    zero_rows = jnp.zeros_like(values[:, :1])
    if offset > 0:
        return jnp.concatenate([values[:, 1:], zero_rows], axis=1)
    return jnp.concatenate([zero_rows, values[:, :-1]], axis=1)

def assemble(latent32, export_nodes):
    exported = jax.vmap(jax.vmap(lambda rows_all, picked: jnp.take(rows_all, picked, axis=0)))(latent32, export_nodes)
    groups = []
    for vertical in (-1, 0, 1):
        for lateral in (-1, 0, 1):
            groups.append(band_shift(jnp.roll(exported, -lateral, axis=0), vertical))
    stacked = jnp.stack(groups, axis=2)
    return stacked.reshape(stacked.shape[:2] + (-1, stacked.shape[-1]))

def give_back(cot_rows):
    slots = cot_rows.reshape(cot_rows.shape[:2] + (3, 3, -1, cot_rows.shape[-1]))
    returned = jnp.zeros(slots.shape[:2] + slots.shape[4:], slots.dtype)
    for vertical in (-1, 0, 1):
        for lateral in (-1, 0, 1):
            moved = jnp.roll(slots[:, :, vertical + 1, lateral + 1], lateral, axis=0)
            returned = returned + band_shift(moved, -vertical)
    return returned

def reference(grid_state, grid_weight, encode_weights, encode_bias, mesh_gain, g2m_sender, g2m_receiver, edge_geometry, edge_embed, mesh_sender, mesh_receiver, block_count, export_nodes, proc_weights, proc_bias, proc_gain, mesh_cotangent):
    device_count = SECTORS * BANDS

    def flatten(values):
        return values.reshape((device_count,) + values.shape[2:])

    def unflatten(values):
        return values.reshape((SECTORS, BANDS) + values.shape[1:])

    def encode_device(entries):
        return encode(entries[0], grid_weight, encode_weights, encode_bias, mesh_gain, entries[1], entries[2], M_DEV)
    latent = lax.map(encode_device, (flatten(grid_state), flatten(g2m_sender), flatten(g2m_receiver)))
    edge_state = lax.map(partial(embed_edges, edge_embed=edge_embed), flatten(edge_geometry))
    block_of_edge = jnp.arange(E_CAP * EDGE_BLOCK, dtype=jnp.int32) // EDGE_BLOCK
    live_mask = (block_of_edge[None, :] < flatten(block_count)[:, None]).astype(jnp.float32)
    senders = flatten(mesh_sender)
    receivers = flatten(mesh_receiver)
    latent32 = lax.optimization_barrier(latent).astype(jnp.float32)
    records = []
    for step_index in range(STEPS):
        halo_rows = flatten(assemble(unflatten(latent32), export_nodes))

        def forward_device(entries):
            return mesh_step(entries[0], entries[1], entries[2], proc_weights[step_index], entries[3], entries[4], entries[5], proc_bias[step_index], proc_gain[step_index])
        new_latent, new_edges = lax.map(forward_device, (latent32, halo_rows, edge_state, senders, receivers, live_mask))
        records.append((latent32, halo_rows, edge_state))
        latent = new_latent.astype(jnp.bfloat16)
        latent32 = lax.optimization_barrier(latent).astype(jnp.float32)
        edge_state = new_edges
    cot_latent = flatten(mesh_cotangent).astype(jnp.float32)
    cot_edges = jnp.zeros_like(edge_state)
    totals = [None] * STEPS
    latent_gradient = None
    for step_index in reversed(range(STEPS)):

        def backward_device(carried, entries):
            local_step = partial(mesh_step, sender=entries[3], receiver=entries[4], live_mask=entries[5], bias=proc_bias[step_index], gain=proc_gain[step_index])
            unused, pullback = jax.vjp(local_step, entries[0], entries[1], entries[2], proc_weights[step_index])
            grad_latent, grad_halo, grad_edges, grad_weights = pullback((entries[6], entries[7]))
            return (carried + grad_weights.astype(jnp.float32), (grad_latent, grad_halo, grad_edges))
        saved_latent, saved_halo, saved_edges = records[step_index]
        summed, outputs = lax.scan(backward_device, jnp.zeros(proc_weights.shape[1:], jnp.float32), (saved_latent, saved_halo, saved_edges, senders, receivers, live_mask, cot_latent, cot_edges))
        grad_latent, grad_halo, grad_edges = outputs
        totals[step_index] = summed
        returned = give_back(unflatten(grad_halo))
        added = jax.vmap(jax.vmap(lambda grads_all, picked, extra_rows: grads_all.at[picked].add(extra_rows)))(unflatten(grad_latent), export_nodes, returned)
        rounded = flatten(added).astype(jnp.bfloat16)
        latent_gradient = rounded
        cot_latent = lax.optimization_barrier(rounded).astype(jnp.float32)
        cot_edges = grad_edges
    weight_grads = jnp.stack(totals).reshape(STEPS, device_count, -1)
    return (unflatten(latent), weight_grads, unflatten(latent_gradient))
```

```python
import jax
import jax.numpy as jnp
from jax import lax
from jax.sharding import PartitionSpec as P

STEPS = 2
EDGE_BLOCK = 256


EPSILON = 1e-05


def padded(x, sides, width, wrap):
    for axis, dim in sides:
        size, length = (lax.axis_size(axis), x.shape[dim])
        up = [(i, (i + 1) % size) for i in range(size if wrap else size - 1)]
        down = [(j, i) for i, j in up]
        last = lax.slice_in_dim(x, length - width, length, axis=dim)
        initial = lax.slice_in_dim(x, 0, width, axis=dim)
        before = lax.ppermute(last, axis, up)
        after = lax.ppermute(initial, axis, down)
        x = jnp.concatenate([before, x, after], axis=dim)
    return x


def layer_norm(values):
    average = jnp.mean(values, axis=-1, keepdims=True)
    centred = values - average
    variance = jnp.mean(centred * centred, axis=-1, keepdims=True)
    return centred * lax.rsqrt(variance + EPSILON)


def encode(
    grid_rows,
    grid_weight,
    encode_weights,
    encode_bias,
    mesh_gain,
    g2m_sender,
    g2m_receiver,
    node_count,
):
    grid_latent = jax.nn.silu(
        jnp.dot(grid_rows, grid_weight, preferred_element_type=jnp.float32)
    ).astype(jnp.bfloat16)
    projected = jnp.dot(grid_latent, encode_weights[0], preferred_element_type=jnp.float32)
    message_act = jax.nn.silu(
        dot32(one_hot(g2m_sender, projected.shape[0]), projected.astype(jnp.bfloat16)) + encode_bias
    ).astype(
        jnp.bfloat16
    )
    message = jnp.dot(message_act, encode_weights[1], preferred_element_type=jnp.float32).astype(
        jnp.bfloat16
    )
    onehot = (g2m_receiver[:, None] == jnp.arange(node_count, dtype=jnp.int32)[None, :]).astype(
        jnp.bfloat16
    )
    gathered = lax.dot_general(
        onehot, message, (((0,), (0,)), ((), ())), preferred_element_type=jnp.float32
    )
    return (layer_norm(gathered) * mesh_gain).astype(jnp.bfloat16)


def embed_edges(geometry, edge_embed):
    product = lax.dot_general(
        geometry,
        edge_embed,
        (((0,), (0,)), ((), ())),
        precision=lax.Precision.HIGHEST,
        preferred_element_type=jnp.float32,
    )
    return product.astype(jnp.bfloat16)


def dot32(x, y, x_dim=1, y_dim=0):
    return lax.dot_general(
        x, y, (((x_dim,), (y_dim,)), ((), ())), preferred_element_type=jnp.float32
    )


def norm_forward(values):
    average = jnp.mean(values, axis=-1, keepdims=True)
    centred = values - average
    scale = lax.rsqrt(jnp.mean(centred * centred, axis=-1, keepdims=True) + EPSILON)
    return centred * scale, scale


def norm_backward(cot, normed, scale):
    first = jnp.mean(cot, axis=-1, keepdims=True)
    second = jnp.mean(cot * normed, axis=-1, keepdims=True)
    return (cot - first - normed * second) * scale


def silu_slope(values):
    gate = jax.nn.sigmoid(values)
    return gate * (1.0 + values * (1.0 - gate))


def step_forward(latent, halo_rows, edge_state, weights, pick, live, bias, gain):
    half = jnp.bfloat16
    nodes, width = latent.shape
    extended = jnp.concatenate([latent, halo_rows], axis=0)
    projected = jnp.concatenate(
        [dot32(extended, weights[1]).astype(half), dot32(latent, weights[2]).astype(half)], axis=0
    )
    before = dot32(edge_state, weights[0]) + dot32(pick, projected) + bias[0]
    edge_act = jax.nn.silu(before).astype(half)
    edge_normed, edge_scale = norm_forward(dot32(edge_act, weights[3]))
    update = edge_normed * gain[0] * live
    new_edges = (edge_state.astype(jnp.float32) + update).astype(half)
    receive = pick[:, -nodes:]
    node_sum = dot32(receive, update.astype(half), 0, 0).astype(half)
    pair = jnp.concatenate([latent, node_sum], axis=1)
    inner = dot32(pair, weights[4:6].reshape(2 * width, width)) + bias[1]
    node_act = jax.nn.silu(inner).astype(half)
    node_normed, node_scale = norm_forward(dot32(node_act, weights[6]))
    new_latent = (latent.astype(jnp.float32) + node_normed * gain[1]).astype(half)
    saved = (
        extended, edge_state, before, edge_act, edge_normed, edge_scale, pair, inner, node_act,
        node_normed, node_scale,
    )
    return new_latent, new_edges, saved


def step_backward(saved, cot_latent, cot_edges, weights, pick, live, gain, want_edges):
    half = jnp.bfloat16
    (
        extended, edge_state, before, edge_act, edge_normed, edge_scale, pair, inner, node_act,
        node_normed, node_scale,
    ) = saved
    nodes, width = cot_latent.shape
    rows = extended.shape[0]
    cot32 = cot_latent.astype(jnp.float32)
    d_out = norm_backward(cot32 * gain[1], node_normed, node_scale).astype(half)
    grad6 = dot32(node_act, d_out, 0, 0)
    d_act = dot32(d_out, weights[6], 1, 1).astype(half).astype(jnp.float32)
    d_inner = (d_act * silu_slope(inner)).astype(half)
    grad45 = dot32(pair, d_inner, 0, 0)
    d_pair = dot32(d_inner, weights[4:6].reshape(2 * width, width), 1, 1).astype(half)
    d_update = dot32(pick[:, -nodes:], d_pair[:, width:])
    if cot_edges is not None:
        d_update = d_update + cot_edges.astype(jnp.float32)
    d_edge_out = norm_backward(d_update * gain[0] * live, edge_normed, edge_scale).astype(half)
    grad3 = dot32(edge_act, d_edge_out, 0, 0)
    d_edge_act = dot32(d_edge_out, weights[3], 1, 1).astype(half).astype(jnp.float32)
    d_before = (d_edge_act * silu_slope(before)).astype(half)
    d_projected = dot32(pick, d_before, 0, 0).astype(half)
    d_extended = dot32(d_projected[:rows], weights[1], 1, 1)
    d_received = dot32(d_projected[rows:], weights[2], 1, 1)
    grad_halo = d_extended[nodes:].astype(half)
    grad_latent = (
        cot32 + d_pair[:, :width].astype(jnp.float32) + d_extended[:nodes] + d_received
    )
    grad0 = dot32(edge_state, d_before, 0, 0)
    grad1 = dot32(extended, d_projected[:rows], 0, 0)
    grad2 = dot32(pair[:, :width], d_projected[rows:], 0, 0)
    grad_weights = jnp.concatenate(
        [g.astype(half) for g in (grad0, grad1, grad2, grad3, grad45, grad6)], axis=0
    )
    grad_edges = dot32(d_before, weights[0], 1, 1).astype(half) if want_edges else None
    return grad_latent, grad_halo, grad_edges, grad_weights


def one_hot(index, count):
    return (index[:, None] == jnp.arange(count, dtype=jnp.int32)[None, :]).astype(jnp.bfloat16)


def shards(
    grid_state,
    grid_weight,
    encode_weights,
    encode_bias,
    mesh_gain,
    g2m_sender,
    g2m_receiver,
    edge_geometry,
    edge_embed,
    mesh_sender,
    mesh_receiver,
    block_count,
    export_nodes,
    proc_weights,
    proc_bias,
    proc_gain,
    mesh_cotangent,
):
    sector_count = lax.axis_size("lon")
    band_count = lax.axis_size("lat")
    node_count = mesh_cotangent.shape[2]
    width = mesh_cotangent.shape[3]
    exporter = export_nodes[0, 0]
    sender = mesh_sender[0, 0]
    receiver = mesh_receiver[0, 0]
    edge_total = sender.shape[0]
    latent = encode(
        grid_state[0, 0],
        grid_weight,
        encode_weights,
        encode_bias,
        mesh_gain,
        g2m_sender[0, 0],
        g2m_receiver[0, 0],
        node_count,
    )
    edge_state = embed_edges(edge_geometry[0, 0], edge_embed)
    block_of_edge = jnp.arange(edge_total, dtype=jnp.int32) // EDGE_BLOCK
    live = (block_of_edge < block_count[0, 0]).astype(jnp.float32)[:, None]
    exported = exporter.shape[0]
    pick = jnp.concatenate(
        [one_hot(sender, node_count + 9 * exported), one_hot(receiver, node_count)], axis=1
    )
    export_pick = one_hot(exporter, node_count)
    records = []
    for step_index in range(STEPS):
        outgoing = dot32(export_pick, latent).astype(jnp.bfloat16)[None]
        sector_rims = padded(outgoing, (("lon", 0),), 1, True)
        beside_all = padded(sector_rims[None], (("lat", 0),), 1, False)
        halo_rows = beside_all.reshape(-1, width)
        latent, edge_state, saved = step_forward(
            latent, halo_rows, edge_state, proc_weights[step_index], pick, live,
            proc_bias[step_index], proc_gain[step_index],
        )
        records.append(saved)
    cot_latent = mesh_cotangent[0, 0]
    cot_edges = None
    collected = [None] * STEPS
    for step_index in reversed(range(STEPS)):
        grad_latent, grad_halo, cot_edges, grad_weights = step_backward(
            records[step_index], cot_latent, cot_edges, proc_weights[step_index], pick, live,
            proc_gain[step_index], step_index > 0,
        )
        collected[step_index] = lax.psum_scatter(
            lax.psum_scatter(grad_weights, "lon", scatter_dimension=0, tiled=True),
            "lat", scatter_dimension=0, tiled=True,
        )
        slot_rows = grad_halo.reshape(3, 3, -1, width)
        lon_rims = padded(slot_rows, (("lon", 1),), 1, True).astype(jnp.float32)
        band_rows = slot_rows[:, 1].astype(jnp.float32) + lon_rims[:, 0] + lon_rims[:, 4]
        lat_rims = padded(band_rows.astype(jnp.bfloat16), (("lat", 0),), 1, False).astype(
            jnp.float32
        )
        returned = band_rows[1] + lat_rims[0] + lat_rims[4]
        grad_latent = grad_latent + dot32(export_pick, returned.astype(jnp.bfloat16), 0, 0)
        cot_latent = grad_latent.astype(jnp.bfloat16)
    weight_grads = jnp.stack(
        [piece.astype(jnp.float32).reshape(1, -1) for piece in collected]
    )
    return (latent[None, None], weight_grads, cot_latent[None, None])


def solution(mesh):
    return jax.shard_map(
        shards,
        mesh=mesh,
        in_specs=(
            P("lon", "lat", None, None),
            P(),
            P(),
            P(),
            P(),
            P("lon", "lat", None),
            P("lon", "lat", None),
            P("lon", "lat", None, None),
            P(),
            P("lon", "lat", None),
            P("lon", "lat", None),
            P("lon", "lat"),
            P("lon", "lat", None),
            P(),
            P(),
            P(),
            P("lon", "lat", None, None),
        ),
        out_specs=(
            P("lon", "lat", None, None),
            P(None, ("lon", "lat"), None),
            P("lon", "lat", None, None),
        ),
        check_vma=False,
    )
```
